16 devices in a mesh: data: 2 (over y, z), pair: 8 (over x, core).
Axes of the slice: x: 4, y: 2, z: 1, core: 2. Of those that a mesh axis runs over, the one named last changes fastest.
The devices are a block of a 4x4x8 slice.
Arguments:
- x_enc: bfloat16 [512, 256, 1024], P(('data', 'pair')), parts along dimension 0
- enc_len: int32 [512], P(('data', 'pair')), parts along dimension 0
- y_dec: bfloat16 [512, 32, 1024], P(('data', 'pair')), parts along dimension 0
- enc_wq: bfloat16 [2, 1024, 1024], replicated
- enc_wk: bfloat16 [2, 1024, 1024], replicated
- enc_wv: bfloat16 [2, 1024, 1024], replicated
- enc_wo: bfloat16 [2, 16, 64, 1024], replicated
- enc_w1: bfloat16 [2, 1024, 2816], replicated
- enc_w2: bfloat16 [2, 2816, 1024], replicated
- dec_wq: bfloat16 [2, 1024, 1024], replicated
- dec_wk: bfloat16 [2, 1024, 1024], replicated
- dec_wv: bfloat16 [2, 1024, 1024], replicated
- dec_wo: bfloat16 [2, 16, 64, 1024], replicated
- crs_wq: bfloat16 [2, 1024, 1024], replicated
- crs_wk: bfloat16 [2, 1024, 1024], replicated
- crs_wv: bfloat16 [2, 1024, 1024], replicated
- crs_wo: bfloat16 [2, 16, 64, 1024], replicated
- dec_w1: bfloat16 [2, 1024, 2816], replicated
- dec_w2: bfloat16 [2, 2816, 1024], replicated
Outputs:
- output: bfloat16 [512, 32, 1024], P(('data', 'pair')), parts along dimension 0
There are 2 independent parts. The reference program is written for one: setup_inputs(seed, part) draws one part's arguments, and reference() takes and returns one part's arrays. A program takes and returns all parts, laid end to end along the dimension named above; an argument that names none is the same for every part.
All inputs are finite; a program needn't handle non-finite values.
Results may differ from the reference program's by a relative error of at most 0.0123475.
Values are sent between devices in bfloat16 or wider.
A program may use at most 768 MiB of HBM per device.

```python
import jax
import jax.numpy as jnp
from jax import lax

BATCH_ROWS = 256
SEQ_ENC = 256
SEQ_DEC = 32
D_MODEL = 1024
NUM_HEADS = 16
KV_HEADS = 16
HEAD_DIM = 64
FF_DIM = 2816
ENC_LAYERS = 2
DEC_LAYERS = 2


def setup_inputs(seed: int = 0, part: int = 0) -> dict:
    base_key = jax.random.key(seed)
    part_key = jax.random.fold_in(base_key, part)
    x_key, y_key = jax.random.split(part_key, 2)
    len_key = jax.random.fold_in(part_key, 3)
    weight_keys = jax.random.split(jax.random.key(seed + 1), 16)
    q_width = NUM_HEADS * HEAD_DIM
    kv_width = KV_HEADS * HEAD_DIM
    in_scale = D_MODEL ** -0.5
    out_scale = q_width ** -0.5
    attn_boost = SEQ_ENC ** 0.5 / 3.0

    def draw_normal(key, shape, scale):
        return (jax.random.normal(key, shape, jnp.float32) * scale).astype(jnp.bfloat16)

    enc_len = jax.random.randint(len_key, (BATCH_ROWS,), SEQ_ENC // 4, SEQ_ENC + 1, dtype=jnp.int32)
    enc_len = enc_len.at[0].set(SEQ_ENC).at[1].set(SEQ_ENC // 4)
    return {
        "x_enc": draw_normal(x_key, (BATCH_ROWS, SEQ_ENC, D_MODEL), 1.0),
        "enc_len": enc_len,
        "y_dec": draw_normal(y_key, (BATCH_ROWS, SEQ_DEC, D_MODEL), 1.0),
        "enc_wq": draw_normal(weight_keys[0], (ENC_LAYERS, D_MODEL, q_width), in_scale),
        "enc_wk": draw_normal(weight_keys[1], (ENC_LAYERS, D_MODEL, kv_width), in_scale),
        "enc_wv": draw_normal(weight_keys[2], (ENC_LAYERS, D_MODEL, kv_width), in_scale),
        "enc_wo": draw_normal(weight_keys[3], (ENC_LAYERS, NUM_HEADS, HEAD_DIM, D_MODEL), out_scale * attn_boost),
        "enc_w1": draw_normal(weight_keys[4], (ENC_LAYERS, D_MODEL, FF_DIM), in_scale),
        "enc_w2": draw_normal(weight_keys[5], (ENC_LAYERS, FF_DIM, D_MODEL), FF_DIM ** -0.5),
        "dec_wq": draw_normal(weight_keys[6], (DEC_LAYERS, D_MODEL, q_width), in_scale),
        "dec_wk": draw_normal(weight_keys[7], (DEC_LAYERS, D_MODEL, kv_width), in_scale),
        "dec_wv": draw_normal(weight_keys[8], (DEC_LAYERS, D_MODEL, kv_width), in_scale),
        "dec_wo": draw_normal(weight_keys[9], (DEC_LAYERS, NUM_HEADS, HEAD_DIM, D_MODEL), out_scale * 1.5),
        "crs_wq": draw_normal(weight_keys[10], (DEC_LAYERS, D_MODEL, q_width), in_scale),
        "crs_wk": draw_normal(weight_keys[11], (DEC_LAYERS, D_MODEL, kv_width), in_scale),
        "crs_wv": draw_normal(weight_keys[12], (DEC_LAYERS, D_MODEL, kv_width), in_scale),
        "crs_wo": draw_normal(weight_keys[13], (DEC_LAYERS, NUM_HEADS, HEAD_DIM, D_MODEL), out_scale * attn_boost),
        "dec_w1": draw_normal(weight_keys[14], (DEC_LAYERS, D_MODEL, FF_DIM), in_scale),
        "dec_w2": draw_normal(weight_keys[15], (DEC_LAYERS, FF_DIM, D_MODEL), FF_DIM ** -0.5),
    }


def rms_norm(hidden):
    x_wide = hidden.astype(jnp.float32)
    inv_rms = lax.rsqrt(jnp.mean(x_wide * x_wide, axis=-1, keepdims=True) + 1e-6)
    return (x_wide * inv_rms).astype(jnp.bfloat16)


def project(source, weight):
    return jnp.dot(source, weight, preferred_element_type=jnp.float32).astype(jnp.bfloat16)


def add_to(hidden, update):
    return (hidden.astype(jnp.float32) + update).astype(jnp.bfloat16)


def attend(query_rows, key_rows, value_rows, allowed, out_weight):
    q_len = query_rows.shape[0]
    k_len = key_rows.shape[0]
    q_heads = query_rows.reshape(q_len, KV_HEADS, NUM_HEADS // KV_HEADS, HEAD_DIM).astype(jnp.float32)
    k_heads = key_rows.reshape(k_len, KV_HEADS, HEAD_DIM).astype(jnp.float32)
    v_heads = value_rows.reshape(k_len, KV_HEADS, HEAD_DIM).astype(jnp.float32)
    scores = jnp.einsum("skrh,tkh->krst", q_heads, k_heads) * HEAD_DIM ** -0.5
    scores = jnp.where(allowed, scores, -1e30)
    attn_probs = jax.nn.softmax(scores, axis=-1).astype(jnp.bfloat16)
    context = jnp.einsum("krst,tkh->skrh", attn_probs.astype(jnp.float32), v_heads).astype(jnp.bfloat16)
    context = context.reshape(q_len, NUM_HEADS * HEAD_DIM)
    w_out = out_weight.reshape(NUM_HEADS * HEAD_DIM, D_MODEL)
    return jnp.dot(context, w_out, preferred_element_type=jnp.float32)


def feed_forward(hidden, w_up, w_down):
    normed = rms_norm(hidden)
    inner_act = jax.nn.gelu(jnp.dot(normed, w_up, preferred_element_type=jnp.float32)).astype(jnp.bfloat16)
    return add_to(hidden, jnp.dot(inner_act, w_down, preferred_element_type=jnp.float32))


def encode_row(x_row, length, enc_weights):
    allowed = jnp.arange(SEQ_ENC)[None, :] < length

    def layer_step(hidden, layer_weights):
        w_query, w_key, w_value, w_out, w_up, w_down = layer_weights
        normed = rms_norm(hidden)
        attn_out = attend(project(normed, w_query), project(normed, w_key), project(normed, w_value), allowed, w_out)
        return feed_forward(add_to(hidden, attn_out), w_up, w_down), None

    hidden, unused = lax.scan(layer_step, x_row, enc_weights)
    return rms_norm(hidden)


def decode_row(y_row, enc_row, length, dec_weights):
    cross_ok = jnp.arange(SEQ_ENC)[None, :] < length
    causal = jnp.arange(SEQ_DEC)[:, None] >= jnp.arange(SEQ_DEC)[None, :]

    def layer_step(hidden, layer_weights):
        w_query, w_key, w_value, w_out, c_query, c_key, c_value, c_out, w_up, w_down = layer_weights
        normed = rms_norm(hidden)
        self_out = attend(project(normed, w_query), project(normed, w_key), project(normed, w_value), causal, w_out)
        hidden = add_to(hidden, self_out)
        normed = rms_norm(hidden)
        cross_out = attend(project(normed, c_query), project(enc_row, c_key), project(enc_row, c_value), cross_ok, c_out)
        return feed_forward(add_to(hidden, cross_out), w_up, w_down), None

    hidden, unused = lax.scan(layer_step, y_row, dec_weights)
    return hidden


def reference(x_enc, enc_len, y_dec, enc_wq, enc_wk, enc_wv, enc_wo, enc_w1, enc_w2, dec_wq, dec_wk, dec_wv, dec_wo, crs_wq, crs_wk, crs_wv, crs_wo, dec_w1, dec_w2):
    enc_weights = (enc_wq, enc_wk, enc_wv, enc_wo, enc_w1, enc_w2)
    dec_weights = (dec_wq, dec_wk, dec_wv, dec_wo, crs_wq, crs_wk, crs_wv, crs_wo, dec_w1, dec_w2)
    enc_out = lax.map(lambda row_in: encode_row(row_in[0], row_in[1], enc_weights), (x_enc, enc_len))
    partner_out = jnp.roll(enc_out, BATCH_ROWS // 2, axis=0)
    partner_len = jnp.roll(enc_len, BATCH_ROWS // 2, axis=0)
    return lax.map(lambda row_in: decode_row(row_in[0], row_in[1], row_in[2], dec_weights), (y_dec, partner_out, partner_len))
```

```python
import functools
import math

import jax
import jax.numpy as jnp
from jax import lax
from jax.experimental import pallas as pl
from jax.experimental.pallas import tpu as pltpu
from jax.sharding import PartitionSpec as P

BF = jnp.bfloat16
F32 = jnp.float32
BLK = 16
TOK = 512
QC = 64
CH = 256
VMEM_LIMIT = 67_043_328
ANY = pl.BlockSpec(memory_space=pl.ANY)


def params(**kw):
    return pltpu.CompilerParams(vmem_limit_bytes=VMEM_LIMIT, **kw)


def dot(a, b):
    return jnp.dot(a, b, preferred_element_type=F32)


def norm(hidden):
    wide = hidden.astype(F32)
    inv = lax.rsqrt(jnp.mean(wide * wide, axis=-1, keepdims=True) + 1e-6)
    return (wide * inv).astype(BF)


def gelu(v):
    return jax.nn.gelu(v, approximate=True)


def quad_masks(head_dim):
    width = 4 * head_dim
    lane = lax.broadcasted_iota(jnp.int32, (1, width), 1) // head_dim
    return [(lane == h).astype(F32).astype(BF) for h in range(4)]


def attend_quad(q, k, v, allowed, head_dim):
    m = q.shape[0]
    masks = quad_masks(head_dim)
    stacked = jnp.concatenate([q * mask for mask in masks], axis=0)
    s = lax.dot_general(stacked, k, (((1,), (1,)), ((), ())), preferred_element_type=F32)
    s = jnp.where(allowed, s, -1e30)
    top = jnp.max(s, axis=-1, keepdims=True)
    p = jnp.exp2((s - top) * (head_dim ** -0.5 * math.log2(math.e)))
    inv = 1.0 / jnp.sum(p, axis=-1, keepdims=True)
    o = dot(p.astype(BF), v)
    low = lax.broadcasted_iota(jnp.int32, (m, 2 * head_dim), 1) < head_dim
    halves = []
    for j in range(2):
        cols = slice(2 * head_dim * j, 2 * head_dim * (j + 1))
        first = o[2 * j * m:(2 * j + 1) * m, cols] * inv[2 * j * m:(2 * j + 1) * m]
        second = o[(2 * j + 1) * m:(2 * j + 2) * m, cols] * inv[(2 * j + 1) * m:(2 * j + 2) * m]
        halves.append(jnp.where(low, first, second).astype(BF))
    return halves


def copies_of(srcs, dsts, sems):
    return [pltpu.make_async_copy(s, d, sems.at[i]) for i, (s, d) in enumerate(zip(srcs, dsts))]


def pack_kernel(layer, src, meta, x_hbm, wq, wk, wv, qkv_out, xp_out, xbuf, sem):
    t, n = pl.program_id(0), meta[0]
    per = TOK // BLK

    def fetch(tile, slot):
        @pl.loop(0, per)
        def _(i):
            row = pl.multiple_of(src[tile * per + i] * BLK, BLK)
            dst = pl.multiple_of(i * BLK, BLK)
            pltpu.make_async_copy(x_hbm.at[pl.ds(row, BLK)], xbuf.at[slot, pl.ds(dst, BLK)], sem.at[slot]).start()

    @pl.when(t == 0)
    def _():
        fetch(0, 0)

    @pl.when(t + 1 < n)
    def _():
        fetch(t + 1, (t + 1) % 2)

    @pl.when(t < n)
    def _():
        slot = t % 2
        pltpu.make_async_copy(x_hbm.at[pl.ds(0, TOK)], xbuf.at[slot], sem.at[slot]).wait()
        x = xbuf[slot]
        xp_out[...] = x
        project(norm(x), (wq, wk, wv), qkv_out)


def project(normed, weights, out):
    width = weights[0].shape[1]
    for i, w in enumerate(weights):
        for c in range(0, width, CH):
            out[:, i * width + c:i * width + c + CH] = dot(normed, w[:, c:c + CH]).astype(BF)


def layer_spec(layer, d0, d1):
    return pl.BlockSpec((None, d0, d1), lambda *_: (layer, 0, 0), pipeline_mode=pl.Buffered(1))


def pack(src, meta, x, weights):
    cap, d = x.shape
    width = weights[0].shape[2]
    tile = lambda t, s, m: (jnp.minimum(t, m[0] - 1), 0)
    return pl.pallas_call(
        functools.partial(pack_kernel, 0),
        grid_spec=pltpu.PrefetchScalarGridSpec(
            num_scalar_prefetch=2, grid=(cap // TOK,),
            in_specs=[ANY] + [layer_spec(0, d, width)] * 3,
            out_specs=[pl.BlockSpec((TOK, 3 * width), tile), pl.BlockSpec((TOK, d), tile)],
            scratch_shapes=[pltpu.VMEM((2, TOK, d), BF), pltpu.SemaphoreType.DMA((2,))]),
        out_shape=[jax.ShapeDtypeStruct((cap + TOK, 3 * width), BF), jax.ShapeDtypeStruct((cap + TOK, d), BF)],
        compiler_params=params(), name="pack_project",
    )(src, meta, x, *weights)


def rows_kernel(head_dim, seq, starts, nblk, lens, qkv_hbm, ctx_hbm, buf, out, vz, sem, osem):
    r, n = pl.program_id(0), pl.num_programs(0)
    d = out.shape[-1]

    def fetch(row, slot):
        return pltpu.make_async_copy(qkv_hbm.at[pl.ds(pl.multiple_of(starts[row] * BLK, BLK), seq)], buf.at[slot], sem.at[slot])

    def put(row, slot, i):
        to = pl.multiple_of((starts[row] + i) * BLK, BLK)
        return pltpu.make_async_copy(out.at[slot, pl.ds(pl.multiple_of(i * BLK, BLK), BLK)], ctx_hbm.at[pl.ds(to, BLK)], osem.at[slot])

    def drain(row, slot):
        @pl.loop(0, nblk[row])
        def _(i):
            put(row, slot, i).wait()

    @pl.when(r == 0)
    def _():
        fetch(0, 0).start()

    @pl.when(r + 1 < n)
    def _():
        fetch(r + 1, (r + 1) % 2).start()

    slot = r % 2

    @pl.when(r >= 2)
    def _():
        drain(r - 2, slot)

    fetch(r, slot).wait()
    length = lens[r]
    keep = lax.broadcasted_iota(jnp.int32, (seq, d), 0) < length
    vz[...] = jnp.where(keep, buf[slot, :, 2 * d:3 * d], jnp.zeros((), BF))
    width = 4 * head_dim

    @pl.loop(0, (length + QC - 1) // QC)
    def _(c):
        rows = pl.ds(pl.multiple_of(c * QC, QC), QC)
        allowed = lax.broadcasted_iota(jnp.int32, (1, seq), 1) < length
        for g in range(d // width):
            lo = g * width
            halves = attend_quad(buf[slot, rows, lo:lo + width], buf[slot, :, d + lo:d + lo + width], vz[:, lo:lo + width], allowed, head_dim)
            for j, half in enumerate(halves):
                out[slot, rows, lo + j * width // 2:lo + (j + 1) * width // 2] = half

    @pl.loop(0, nblk[r])
    def _(i):
        put(r, slot, i).start()

    @pl.when(r == n - 1)
    def _():
        drain(r - 1, 1 - slot)
        drain(r, slot)


def attend_rows(starts, nblk, lens, qkv, seq, head_dim):
    d = qkv.shape[1] // 3
    return pl.pallas_call(
        functools.partial(rows_kernel, head_dim, seq),
        grid_spec=pltpu.PrefetchScalarGridSpec(
            num_scalar_prefetch=3, grid=(lens.shape[0],), in_specs=[ANY], out_specs=ANY,
            scratch_shapes=[pltpu.VMEM((2, seq, 3 * d), BF), pltpu.VMEM((2, seq, d), BF), pltpu.VMEM((seq, d), BF),
                            pltpu.SemaphoreType.DMA((2,)), pltpu.SemaphoreType.DMA((2,))]),
        out_shape=jax.ShapeDtypeStruct((qkv.shape[0], d), BF),
        compiler_params=params(), name="row_attention",
    )(starts, nblk, lens, qkv)


def dense_block(ctx, x, wo, w1, w2, hid, inner, need):
    d = hid.shape[1]
    need(0)
    for c in range(0, d, CH):
        hid[:, c:c + CH] = (x[:, c:c + CH].astype(F32) + dot(ctx[...], wo[:, c:c + CH])).astype(BF)
    ffn(hid, w1, w2, inner, need)


def ffn(hid, w1, w2, inner, need):
    d, ff = w1.shape
    need(1)
    normed = norm(hid[...])
    for c in range(0, ff, CH):
        inner[:, c:c + CH] = gelu(dot(normed, w1[:, c:c + CH])).astype(BF)
    need(2)
    for c in range(0, d, CH):
        hid[:, c:c + CH] = (hid[:, c:c + CH].astype(F32) + dot(inner[...], w2[:, c:c + CH])).astype(BF)


def mid_kernel(layer, nxt, meta, ctx, x, wo_h, w1_h, w2_h, wq_h, wk_h, wv_h, h_out, qkv_out, wo, w1, w2, wq, wk, wv, inner, sem):
    t, n = pl.program_id(0), meta[0]
    loads = copies_of([wo_h.at[layer], w1_h.at[layer], w2_h.at[layer], wq_h.at[nxt], wk_h.at[nxt], wv_h.at[nxt]], [wo, w1, w2, wq, wk, wv], sem)

    @pl.when(t == 0)
    def _():
        for load in loads:
            load.start()

    def need(*which):
        @pl.when(t == 0)
        def _():
            for i in which:
                loads[i].wait()

    @pl.when(t < n)
    def _():
        dense_block(ctx, x, wo, w1, w2, h_out, inner, need)
        need(3, 4, 5)
        project(norm(h_out[...]), (wq, wk, wv), qkv_out)


def mid(layer, nxt, meta, ctx, x, wo, w1, w2, wq, wk, wv):
    cap, d = x.shape
    ff, width = w1.shape[2], wq.shape[2]
    tile = lambda t, m: (jnp.minimum(t, m[0] - 1), 0)
    return pl.pallas_call(
        functools.partial(mid_kernel, layer, nxt),
        grid_spec=pltpu.PrefetchScalarGridSpec(
            num_scalar_prefetch=1, grid=(cap // TOK - 1,),
            in_specs=[pl.BlockSpec((TOK, d), tile), pl.BlockSpec((TOK, d), tile)] + [ANY] * 6,
            out_specs=[pl.BlockSpec((TOK, d), tile), pl.BlockSpec((TOK, 3 * width), tile)],
            scratch_shapes=[pltpu.VMEM((d, d), BF), pltpu.VMEM((d, ff), BF), pltpu.VMEM((ff, d), BF)] + [pltpu.VMEM((d, width), BF)] * 3
            + [pltpu.VMEM((TOK, ff), BF), pltpu.SemaphoreType.DMA((6,))]),
        out_shape=[jax.ShapeDtypeStruct((cap, d), BF), jax.ShapeDtypeStruct((cap, 3 * width), BF)],
        compiler_params=params(), name="mid_dense",
    )(meta, ctx, x, wo, w1, w2, wq, wk, wv)


def last_kernel(layer, n_dec, src, meta, ctx, x, wo_h, w1_h, w2_h, ck_h, cv_h, kv_hbm, wo, w1, w2, ckv, hid, inner, kv, sem, osem):
    t, n, total = pl.program_id(0), meta[0], meta[1]
    per = TOK // BLK
    crs = [h.at[l] for l in range(n_dec) for h in (ck_h, cv_h)]
    loads = copies_of([wo_h.at[layer], w1_h.at[layer], w2_h.at[layer]] + crs, [wo, w1, w2] + [ckv.at[i] for i in range(2 * n_dec)], sem)

    @pl.when(t == 0)
    def _():
        for load in loads:
            load.start()

    def need(*which):
        @pl.when(t == 0)
        def _():
            for i in which:
                loads[i].wait()

    def put(tile, i):
        to = pl.multiple_of(src[tile * per + i] * BLK, BLK)
        return pltpu.make_async_copy(kv.at[pl.ds(pl.multiple_of(i * BLK, BLK), BLK)], kv_hbm.at[pl.ds(to, BLK)], osem)

    def drain(tile):
        @pl.loop(0, jnp.minimum(per, total - tile * per))
        def _(i):
            put(tile, i).wait()

    @pl.when(t < n)
    def _():
        dense_block(ctx, x, wo, w1, w2, hid, inner, need)
        need(*range(3, 3 + 2 * n_dec))

        @pl.when(t > 0)
        def _():
            drain(t - 1)

        project(norm(hid[...]), [ckv.at[i] for i in range(2 * n_dec)], kv)

        @pl.loop(0, jnp.minimum(per, total - t * per))
        def _(i):
            put(t, i).start()

        @pl.when(t == n - 1)
        def _():
            drain(t)


def last(layer, src, meta, ctx, x, wo, w1, w2, ck, cv, slots):
    cap, d = x.shape
    n_dec, ff, width = ck.shape[0], w1.shape[2], ck.shape[2]
    tile = lambda t, s, m: (jnp.minimum(t, m[0] - 1), 0)
    return pl.pallas_call(
        functools.partial(last_kernel, layer, n_dec),
        grid_spec=pltpu.PrefetchScalarGridSpec(
            num_scalar_prefetch=2, grid=(cap // TOK - 1,),
            in_specs=[pl.BlockSpec((TOK, d), tile), pl.BlockSpec((TOK, d), tile)] + [ANY] * 5,
            out_specs=ANY,
            scratch_shapes=[pltpu.VMEM((d, d), BF), pltpu.VMEM((d, ff), BF), pltpu.VMEM((ff, d), BF), pltpu.VMEM((2 * n_dec, d, width), BF),
                            pltpu.VMEM((TOK, d), BF), pltpu.VMEM((TOK, ff), BF), pltpu.VMEM((TOK, 2 * n_dec * width), BF),
                            pltpu.SemaphoreType.DMA((3 + 2 * n_dec,)), pltpu.SemaphoreType.DMA]),
        out_shape=jax.ShapeDtypeStruct((slots, 2 * n_dec * width), BF),
        compiler_params=params(), name="last_dense",
    )(src, meta, ctx, x, wo, w1, w2, ck, cv)


def dec_kernel(head_dim, seq, dec_len, lens, y, kv_hbm, *refs):
    hbm_w, refs = refs[:8], refs[8:]
    out, refs = refs[0], refs[1:]
    vmem_w, (hid, qkv, ctx, inner, kv, vz, sem, ksem) = refs[:8], refs[8:]
    n_dec = vmem_w[0].shape[0]
    t = pl.program_id(0)
    m, d = hid.shape
    per = m // dec_len
    width = 4 * head_dim
    loads = []
    for l in range(n_dec):
        loads += [pltpu.make_async_copy(h.at[l], v.at[l], sem.at[l * 8 + i]) for i, (h, v) in enumerate(zip(hbm_w, vmem_w))]

    def need(l, *which):
        @pl.when(t == 0)
        def _():
            for i in which:
                loads[l * 8 + i].wait()

    def fetch(l, i, slot):
        rows = pl.ds(pl.multiple_of((t * per + i) * seq, seq), seq)
        return pltpu.make_async_copy(kv_hbm.at[rows, pl.ds(2 * d * l, 2 * d)], kv.at[slot], ksem.at[slot])

    @pl.when(t == 0)
    def _():
        for load in loads:
            load.start()

    hid[...] = y[...]
    row_q = lax.broadcasted_iota(jnp.int32, (4 * m, m), 0) % m
    col_k = lax.broadcasted_iota(jnp.int32, (4 * m, m), 1)
    causal = (row_q >= col_k) & (row_q // dec_len == col_k // dec_len)
    wq, wk, wv, wo, cq, co, w1, w2 = vmem_w
    for l in range(n_dec):
        fetch(l, 0, 0).start()
        need(l, 0, 1, 2)
        project(norm(hid[...]), (wq.at[l], wk.at[l], wv.at[l]), qkv)
        for g in range(d // width):
            lo = g * width
            halves = attend_quad(qkv[:, lo:lo + width], qkv[:, d + lo:d + lo + width], qkv[:, 2 * d + lo:2 * d + lo + width], causal, head_dim)
            for j, half in enumerate(halves):
                ctx[:, lo + j * width // 2:lo + (j + 1) * width // 2] = half
        need(l, 3, 4)
        for c in range(0, d, CH):
            hid[:, c:c + CH] = (hid[:, c:c + CH].astype(F32) + dot(ctx[...], wo[l, :, c:c + CH])).astype(BF)
        project(norm(hid[...]), (cq.at[l],), qkv)

        @pl.loop(0, per)
        def _(i):
            slot = i % 2

            @pl.when(i + 1 < per)
            def _():
                fetch(l, i + 1, 1 - slot).start()

            fetch(l, i, slot).wait()
            length = lens[t * per + i]
            vz[...] = jnp.where(lax.broadcasted_iota(jnp.int32, (seq, d), 0) < length, kv[slot, :, d:2 * d], jnp.zeros((), BF))
            allowed = lax.broadcasted_iota(jnp.int32, (1, seq), 1) < length
            rows = pl.ds(pl.multiple_of(i * dec_len, dec_len), dec_len)
            for g in range(d // width):
                lo = g * width
                halves = attend_quad(qkv[rows, lo:lo + width], kv[slot, :, lo:lo + width], vz[:, lo:lo + width], allowed, head_dim)
                for j, half in enumerate(halves):
                    ctx[rows, lo + j * width // 2:lo + (j + 1) * width // 2] = half

        need(l, 5)
        for c in range(0, d, CH):
            hid[:, c:c + CH] = (hid[:, c:c + CH].astype(F32) + dot(ctx[...], co[l, :, c:c + CH])).astype(BF)
        ffn(hid, w1.at[l], w2.at[l], inner, lambda i: need(l, 5 + i))
    out[...] = hid[...]


def decode(lens, y, kv, weights, seq, dec_len, head_dim, chunk):
    toks, d = y.shape
    ff = weights[6].shape[2]
    return pl.pallas_call(
        functools.partial(dec_kernel, head_dim, seq, dec_len),
        grid_spec=pltpu.PrefetchScalarGridSpec(
            num_scalar_prefetch=1, grid=(toks // chunk,),
            in_specs=[pl.BlockSpec((chunk, d), lambda t, s: (t, 0))] + [ANY] * 9,
            out_specs=pl.BlockSpec((chunk, d), lambda t, s: (t, 0)),
            scratch_shapes=[pltpu.VMEM(w.shape, BF) for w in weights]
            + [pltpu.VMEM((chunk, d), BF), pltpu.VMEM((chunk, 3 * d), BF), pltpu.VMEM((chunk, d), BF), pltpu.VMEM((chunk, ff), BF),
               pltpu.VMEM((2, seq, 2 * d), BF), pltpu.VMEM((seq, d), BF),
               pltpu.SemaphoreType.DMA((8 * weights[0].shape[0],)), pltpu.SemaphoreType.DMA((2,))]),
        out_shape=jax.ShapeDtypeStruct((toks, d), BF),
        compiler_params=params(), name="decoder",
    )(lens, y, kv, *weights)


def solution(mesh):
    pair_size = mesh.shape["pair"]
    to_partner = [(source, (source + pair_size // 2) % pair_size) for source in range(pair_size)]
    row_spec = P(("data", "pair"))

    def per_device(x_enc, enc_len, y_dec, enc_wq, enc_wk, enc_wv, enc_wo, enc_w1, enc_w2, dec_wq, dec_wk, dec_wv, dec_wo, crs_wq, crs_wk, crs_wv, crs_wo, dec_w1, dec_w2):
        rows, seq, d = x_enc.shape
        dec_len = y_dec.shape[1]
        head_dim = enc_wo.shape[2]
        flat = lambda w: w.reshape(w.shape[0], w.shape[1] * w.shape[2], w.shape[3])
        enc_wo, dec_wo, crs_wo = flat(enc_wo), flat(dec_wo), flat(crs_wo)
        y_in = lax.ppermute(y_dec.reshape(rows * dec_len, d), "pair", to_partner)

        nblk = (enc_len + BLK - 1) // BLK
        ends = jnp.cumsum(nblk)
        starts = ends - nblk
        total = ends[-1]
        blk = jnp.arange(rows * seq // BLK, dtype=jnp.int32)
        row_of = jnp.minimum(jnp.sum((ends[None, :] <= blk[:, None]).astype(jnp.int32), axis=1), rows - 1)
        first = jnp.sum(jnp.where(row_of[:, None] == jnp.arange(rows)[None, :], starts[None, :], 0), axis=1)
        src = jnp.where(blk < total, row_of * (seq // BLK) + blk - first, 0)
        meta = jnp.stack([(total * BLK + TOK - 1) // TOK, total])

        x_flat = x_enc.reshape(rows * seq, d)
        n_enc = enc_wq.shape[0]
        qkv, h = pack(src, meta, x_flat, (enc_wq, enc_wk, enc_wv))
        for l in range(n_enc):
            ctx = attend_rows(starts, nblk, enc_len, qkv, seq, head_dim)
            if l + 1 < n_enc:
                h, qkv = mid(l, l + 1, meta, ctx, h, enc_wo, enc_w1, enc_w2, enc_wq, enc_wk, enc_wv)
            else:
                kv = last(l, src, meta, ctx, h, enc_wo, enc_w1, enc_w2, crs_wk, crs_wv, rows * seq)
        z = decode(enc_len, y_in, kv, (dec_wq, dec_wk, dec_wv, dec_wo, crs_wq, crs_wo, dec_w1, dec_w2), seq, dec_len, head_dim, 8 * dec_len)
        return lax.ppermute(z, "pair", to_partner).reshape(y_dec.shape)

    return jax.shard_map(per_device, mesh=mesh, in_specs=(row_spec,) * 3 + (P(),) * 16, out_specs=row_spec, check_vma=False)
```

```python
import functools
import math

import jax
import jax.numpy as jnp
from jax import lax
from jax.experimental import pallas as pl
from jax.experimental.pallas import tpu as pltpu
from jax.sharding import PartitionSpec as P

BF = jnp.bfloat16
F32 = jnp.float32
BLK = 16
TOK = 512
QC = 128
CH = 256
AHEAD = 1
AHEAD_S = 2
AHEAD_C = 7
PAIR = 2
GRP = 128
CHUNK = 8
VMEM_LIMIT = 67_043_328
ANY = pl.BlockSpec(memory_space=pl.ANY)


def params(**kw):
    return pltpu.CompilerParams(vmem_limit_bytes=VMEM_LIMIT, **kw)


def dot(a, b):
    return jnp.dot(a, b, preferred_element_type=F32)


def norm(hidden):
    wide = hidden.astype(F32)
    inv = lax.rsqrt(jnp.mean(wide * wide, axis=-1, keepdims=True) + 1e-6)
    return (wide * inv).astype(BF)


def gelu(v):
    return jax.nn.gelu(v, approximate=True)


def quad_masks(head_dim):
    width = 4 * head_dim
    lane = lax.broadcasted_iota(jnp.int32, (1, width), 1) // head_dim
    return [(lane == h).astype(F32).astype(BF) for h in range(4)]


def quad_scores(q, k, head_dim):
    stacked = jnp.concatenate([q * mask for mask in quad_masks(head_dim)], axis=0)
    return lax.dot_general(stacked, k, (((1,), (1,)), ((), ())), preferred_element_type=F32)


def quad_context(s, v, allowed, head_dim):
    m = s.shape[0] // 4
    s = jnp.where(allowed, s, -1e30)
    top = jnp.max(s, axis=-1, keepdims=True)
    p = jnp.exp2((s - top) * (head_dim ** -0.5 * math.log2(math.e)))
    inv = 1.0 / jnp.sum(p, axis=-1, keepdims=True)
    o = dot(p.astype(BF), v)
    low = lax.broadcasted_iota(jnp.int32, (m, 2 * head_dim), 1) < head_dim
    halves = []
    for j in range(2):
        cols = slice(2 * head_dim * j, 2 * head_dim * (j + 1))
        first = o[2 * j * m:(2 * j + 1) * m, cols] * inv[2 * j * m:(2 * j + 1) * m]
        second = o[(2 * j + 1) * m:(2 * j + 2) * m, cols] * inv[(2 * j + 1) * m:(2 * j + 2) * m]
        halves.append(jnp.where(low, first, second).astype(BF))
    return halves


def attend_all(units, head_dim, ahead):
    held = {}
    for i in range(len(units) + ahead):
        if i < len(units):
            q, k = units[i][:2]
            held[i] = quad_scores(q(), k(), head_dim)
        if i >= ahead:
            v, allowed, store = units[i - ahead][2:]
            for j, half in enumerate(quad_context(held.pop(i - ahead), v(), allowed, head_dim)):
                store(j, half)


class Loader:
    def __init__(self, srcs, dsts, sems, ahead):
        self.loads = [pltpu.make_async_copy(s, d, sems.at[i]) for i, (s, d) in enumerate(zip(srcs, dsts))]
        self.ahead, self.started, self.waited = ahead, 0, 0
        self.first = pl.program_id(0) == 0

    def start(self, upto):
        for i in range(self.started, min(upto, len(self.loads))):
            self.loads[i].start()
        self.started = max(self.started, min(upto, len(self.loads)))

    def need(self, upto):
        @pl.when(self.first)
        def _():
            self.start(upto)
            for i in range(self.waited, upto):
                self.loads[i].wait()
            self.start(upto + self.ahead)
        self.waited = upto


def pack_kernel(layer, src, meta, x_hbm, wq, wk, wv, qkv_out, xp_out, xbuf, sem):
    t, n = pl.program_id(0), meta[0]
    per = TOK // BLK

    def fetch(tile, slot):
        @pl.loop(0, per)
        def _(i):
            row = pl.multiple_of(src[tile * per + i] * BLK, BLK)
            dst = pl.multiple_of(i * BLK, BLK)
            pltpu.make_async_copy(x_hbm.at[pl.ds(row, BLK)], xbuf.at[slot, pl.ds(dst, BLK)], sem.at[slot]).start()

    @pl.when(t == 0)
    def _():
        fetch(0, 0)

    @pl.when(t + 1 < n)
    def _():
        fetch(t + 1, (t + 1) % 2)

    @pl.when(t < n)
    def _():
        slot = t % 2
        pltpu.make_async_copy(x_hbm.at[pl.ds(0, TOK)], xbuf.at[slot], sem.at[slot]).wait()
        xp_out[...] = xbuf[slot]

        def run(part, _):
            project(norm(xbuf[slot, part, :]), (wq, wk, wv), qkv_out, part)

        by_fill(t, meta[1], run)


def by_fill(t, total, run):
    whole = (t + 1) * TOK - TOK // 2 < total * BLK

    @pl.when(whole)
    def _():
        run(slice(0, TOK), True)

    @pl.when(jnp.logical_not(whole))
    def _():
        run(slice(0, TOK // 2), False)


def project(normed, weights, out, part=slice(None)):
    width = weights[0].shape[1]
    for i, w in enumerate(weights):
        for c in range(0, width, CH):
            out[part, i * width + c:i * width + c + CH] = dot(normed, w[:, c:c + CH]).astype(BF)


def layer_spec(layer, d0, d1):
    return pl.BlockSpec((None, d0, d1), lambda *_: (layer, 0, 0), pipeline_mode=pl.Buffered(1))


def pack(src, meta, x, weights):
    cap, d = x.shape
    width = weights[0].shape[2]
    tile = lambda t, s, m: (jnp.minimum(t, m[0] - 1), 0)
    return pl.pallas_call(
        functools.partial(pack_kernel, 0),
        grid_spec=pltpu.PrefetchScalarGridSpec(
            num_scalar_prefetch=2, grid=(cap // TOK,),
            in_specs=[ANY] + [layer_spec(0, d, width)] * 3,
            out_specs=[pl.BlockSpec((TOK, 3 * width), tile), pl.BlockSpec((TOK, d), tile)],
            scratch_shapes=[pltpu.VMEM((2, TOK, d), BF), pltpu.SemaphoreType.DMA((2,))]),
        out_shape=[jax.ShapeDtypeStruct((cap + TOK, 3 * width), BF), jax.ShapeDtypeStruct((cap + TOK, d), BF)],
        compiler_params=params(), name="pack_project",
    )(src, meta, x, *weights)


def pieces(count, make):
    for size in (16, 8, 4, 2, 1):
        @pl.when((count & size) != 0)
        def _(size=size):
            make(count - (count & (2 * size - 1)), size)


def rows_kernel(head_dim, seq, starts, nblk, lens, qkv_hbm, ctx_hbm, buf, out, sem, osem):
    r, n = pl.program_id(0), pl.num_programs(0)
    d = out.shape[-1]

    def fetch(row, slot):
        return pltpu.make_async_copy(qkv_hbm.at[pl.ds(pl.multiple_of(starts[row] * BLK, BLK), seq)], buf.at[slot], sem.at[slot])

    def put(row, slot, first, size):
        to = pl.multiple_of((starts[row] + first) * BLK, BLK)
        frm = pl.multiple_of(first * BLK, BLK)
        return pltpu.make_async_copy(out.at[slot, pl.ds(frm, size * BLK)], ctx_hbm.at[pl.ds(to, size * BLK)], osem.at[slot])

    def drain(row, slot):
        pieces(nblk[row], lambda first, size: put(row, slot, first, size).wait())

    @pl.when(r == 0)
    def _():
        fetch(0, 0).start()

    @pl.when(r + 1 < n)
    def _():
        fetch(r + 1, (r + 1) % 2).start()

    slot = r % 2

    @pl.when(r >= 2)
    def _():
        drain(r - 2, slot)

    fetch(r, slot).wait()
    length = lens[r]

    @pl.when(starts[r] + seq // BLK > starts[n - 1] + nblk[n - 1])
    def _():
        keep = lax.broadcasted_iota(jnp.int32, (seq, d), 0) < length
        buf[slot, :, 2 * d:3 * d] = jnp.where(keep, buf[slot, :, 2 * d:3 * d], jnp.zeros((), BF))

    width = 4 * head_dim

    @pl.loop(0, (length + QC - 1) // QC)
    def _(c):
        rows = pl.ds(pl.multiple_of(c * QC, QC), QC)
        allowed = lax.broadcasted_iota(jnp.int32, (1, seq), 1) < length
        units = []
        for g in range(d // width):
            def store(j, half, lo=g * width):
                out[slot, rows, lo + j * width // 2:lo + (j + 1) * width // 2] = half
            lo = g * width
            units.append((lambda lo=lo: buf[slot, rows, lo:lo + width], lambda lo=lo: buf[slot, :, d + lo:d + lo + width],
                          lambda lo=lo: buf[slot, :, 2 * d + lo:2 * d + lo + width], allowed, store))
        attend_all(units, head_dim, AHEAD)

    pieces(nblk[r], lambda first, size: put(r, slot, first, size).start())

    @pl.when(r == n - 1)
    def _():
        drain(r - 1, 1 - slot)
        drain(r, slot)


def attend_rows(starts, nblk, lens, qkv, seq, head_dim):
    d = qkv.shape[1] // 3
    return pl.pallas_call(
        functools.partial(rows_kernel, head_dim, seq),
        grid_spec=pltpu.PrefetchScalarGridSpec(
            num_scalar_prefetch=3, grid=(lens.shape[0],), in_specs=[ANY], out_specs=ANY,
            scratch_shapes=[pltpu.VMEM((2, seq, 3 * d), BF), pltpu.VMEM((2, seq, d), BF),
                            pltpu.SemaphoreType.DMA((2,)), pltpu.SemaphoreType.DMA((2,))]),
        out_shape=jax.ShapeDtypeStruct((qkv.shape[0], d), BF),
        compiler_params=params(), name="row_attention",
    )(starts, nblk, lens, qkv)


def up(normed, w1, inner, part):
    for c in range(0, w1.shape[1], CH):
        inner[part, c:c + CH] = gelu(dot(normed, w1[:, c:c + CH])).astype(BF)


def add_dot(base, source, w, hid, part):
    for c in range(0, hid.shape[1], CH):
        hid[part, c:c + CH] = (base[part, c:c + CH].astype(F32) + dot(source[part, :], w[:, c:c + CH])).astype(BF)


def dense_part(part, ctx, x, wo, w1, w2, hid, inner, nxt, out, need):
    need(0)
    add_dot(x, ctx, wo, hid, part)
    need(1)
    up(norm(hid[part, :]), w1, inner, part)
    need(2)
    add_dot(hid, inner, w2, hid, part)
    need(3)
    project(norm(hid[part, :]), nxt, out, part)


def mid_kernel(layer, nxt, meta, ctx, x, wo_h, w1_h, w2_h, wq_h, wk_h, wv_h, h_out, qkv_out, wo, w1, w2, wq, wk, wv, inner, sem):
    t, n = pl.program_id(0), meta[0]
    loader = Loader([wo_h.at[layer], w1_h.at[layer], w2_h.at[layer], wq_h.at[nxt], wk_h.at[nxt], wv_h.at[nxt]], [wo, w1, w2, wq, wk, wv], sem, 4)

    @pl.when(t == 0)
    def _():
        loader.start(2)

    counts = [1, 2, 3, 6]

    def run(part, whole):
        dense_part(part, ctx, x, wo, w1, w2, h_out, inner, (wq, wk, wv), qkv_out, lambda i: loader.need(counts[i]) if whole else None)

    @pl.when(t < n)
    def _():
        by_fill(t, meta[1], run)


def mid(layer, nxt, meta, ctx, x, wo, w1, w2, wq, wk, wv):
    cap, d = x.shape
    ff, width = w1.shape[2], wq.shape[2]
    tile = lambda t, m: (jnp.minimum(t, m[0] - 1), 0)
    return pl.pallas_call(
        functools.partial(mid_kernel, layer, nxt),
        grid_spec=pltpu.PrefetchScalarGridSpec(
            num_scalar_prefetch=1, grid=(cap // TOK - 1,),
            in_specs=[pl.BlockSpec((TOK, d), tile), pl.BlockSpec((TOK, d), tile)] + [ANY] * 6,
            out_specs=[pl.BlockSpec((TOK, d), tile), pl.BlockSpec((TOK, 3 * width), tile)],
            scratch_shapes=[pltpu.VMEM((d, d), BF), pltpu.VMEM((d, ff), BF), pltpu.VMEM((ff, d), BF)] + [pltpu.VMEM((d, width), BF)] * 3
            + [pltpu.VMEM((TOK, ff), BF), pltpu.SemaphoreType.DMA((6,))]),
        out_shape=[jax.ShapeDtypeStruct((cap, d), BF), jax.ShapeDtypeStruct((cap, 3 * width), BF)],
        compiler_params=params(), name="mid_dense",
    )(meta, ctx, x, wo, w1, w2, wq, wk, wv)


def last_kernel(layer, n_dec, src, meta, ctx, x, wo_h, w1_h, w2_h, ck_h, cv_h, kv_hbm, wo, w1, w2, ckv, hid, inner, kv, sem, osem):
    t, n, total = pl.program_id(0), meta[0], meta[1]
    per = TOK // BLK
    crs = [h.at[l] for l in range(n_dec) for h in (ck_h, cv_h)]
    nxt = [ckv.at[i] for i in range(2 * n_dec)]
    loader = Loader([wo_h.at[layer], w1_h.at[layer], w2_h.at[layer]] + crs, [wo, w1, w2] + nxt, sem, 4)

    @pl.when(t == 0)
    def _():
        loader.start(2)

    def put(tile, i):
        to = pl.multiple_of(src[tile * per + i] * BLK, BLK)
        return pltpu.make_async_copy(kv.at[pl.ds(pl.multiple_of(i * BLK, BLK), BLK)], kv_hbm.at[pl.ds(to, BLK)], osem)

    def drain(tile):
        @pl.loop(0, jnp.minimum(per, total - tile * per))
        def _(i):
            put(tile, i).wait()

    counts = [1, 2, 3, 3 + 2 * n_dec]

    def run(part, whole):
        def need(i):
            if whole:
                loader.need(counts[i])
            if i == 3:
                @pl.when(t > 0)
                def _():
                    drain(t - 1)

        dense_part(part, ctx, x, wo, w1, w2, hid, inner, nxt, kv, need)

    @pl.when(t < n)
    def _():
        by_fill(t, total, run)

        @pl.loop(0, jnp.minimum(per, total - t * per))
        def _(i):
            put(t, i).start()

        @pl.when(t == n - 1)
        def _():
            drain(t)


def last(layer, src, meta, ctx, x, wo, w1, w2, ck, cv, slots):
    cap, d = x.shape
    n_dec, ff, width = ck.shape[0], w1.shape[2], ck.shape[2]
    tile = lambda t, s, m: (jnp.minimum(t, m[0] - 1), 0)
    return pl.pallas_call(
        functools.partial(last_kernel, layer, n_dec),
        grid_spec=pltpu.PrefetchScalarGridSpec(
            num_scalar_prefetch=2, grid=(slots // TOK,),
            in_specs=[pl.BlockSpec((TOK, d), tile), pl.BlockSpec((TOK, d), tile)] + [ANY] * 5,
            out_specs=ANY,
            scratch_shapes=[pltpu.VMEM((d, d), BF), pltpu.VMEM((d, ff), BF), pltpu.VMEM((ff, d), BF), pltpu.VMEM((2 * n_dec, d, width), BF),
                            pltpu.VMEM((TOK, d), BF), pltpu.VMEM((TOK, ff), BF), pltpu.VMEM((TOK, 2 * n_dec * width), BF),
                            pltpu.SemaphoreType.DMA((3 + 2 * n_dec,)), pltpu.SemaphoreType.DMA]),
        out_shape=jax.ShapeDtypeStruct((slots, 2 * n_dec * width), BF),
        compiler_params=params(), name="last_dense",
    )(src, meta, ctx, x, wo, w1, w2, ck, cv)


def dec_kernel(head_dim, seq, dec_len, first_row, lens, nblk, y, kv_hbm, *refs):
    hbm_w, refs = refs[:8], refs[8:]
    out, refs = refs[0], refs[1:]
    vmem_w, (hid, qkv, ctx, inner, kv, sem, ksem) = refs[:8], refs[8:]
    n_dec = vmem_w[0].shape[0]
    t = pl.program_id(0)
    m, d = hid.shape
    per = m // dec_len
    width = 4 * head_dim
    srcs, dsts = [], []
    for l in range(n_dec):
        srcs += [h.at[l] for h in hbm_w]
        dsts += [v.at[l] for v in vmem_w]
    loader = Loader(srcs, dsts, sem, 3)

    def fetch(l, pair, slot, act):
        for u in range(PAIR):
            row = first_row + t * per + pair * PAIR + u

            def one(first, size, row=row, u=u):
                frm = pl.multiple_of(row * seq + first * BLK, BLK)
                to = pl.multiple_of(first * BLK, BLK)
                getattr(pltpu.make_async_copy(kv_hbm.at[pl.ds(frm, size * BLK), pl.ds(2 * d * l, 2 * d)], kv.at[slot, u, pl.ds(to, size * BLK)], ksem.at[slot, u]), act)()

            pieces(nblk[row], one)

    @pl.when(t == 0)
    def _():
        loader.start(5)
        kv[...] = jnp.zeros_like(kv)

    hid[...] = y[...]
    row_q = lax.broadcasted_iota(jnp.int32, (4 * GRP, GRP), 0) % GRP
    col_k = lax.broadcasted_iota(jnp.int32, (4 * GRP, GRP), 1)
    causal = (row_q >= col_k) & (row_q // dec_len == col_k // dec_len)
    wq, wk, wv, wo, cq, co, w1, w2 = vmem_w
    for l in range(n_dec):
        fetch(l, 0, 0, "start")
        loader.need(8 * l + 3)
        project(norm(hid[...]), (wq.at[l], wk.at[l], wv.at[l]), qkv)
        units = []
        for lo in range(0, d, width):
            for r0 in range(0, m, GRP):
                def store(j, half, lo=lo, r0=r0):
                    ctx[r0:r0 + GRP, lo + j * width // 2:lo + (j + 1) * width // 2] = half
                read = lambda at, r0=r0: (lambda: qkv[r0:r0 + GRP, at:at + width])
                units.append((read(lo), read(d + lo), read(2 * d + lo), causal, store))
        attend_all(units, head_dim, AHEAD_S)
        loader.need(8 * l + 5)
        for c in range(0, d, CH):
            hid[:, c:c + CH] = (hid[:, c:c + CH].astype(F32) + dot(ctx[...], wo[l, :, c:c + CH])).astype(BF)
        project(norm(hid[...]), (cq.at[l],), qkv)

        @pl.loop(0, per // PAIR)
        def _(i):
            slot = i % 2

            @pl.when(i + 1 < per // PAIR)
            def _():
                fetch(l, i + 1, 1 - slot, "start")

            fetch(l, i, slot, "wait")
            units = []
            for u in range(PAIR):
                length = lens[first_row + t * per + i * PAIR + u]
                allowed = lax.broadcasted_iota(jnp.int32, (1, seq), 1) < length
                rows = pl.ds(pl.multiple_of((i * PAIR + u) * dec_len, dec_len), dec_len)
                for lo in range(0, d, width):
                    def store(j, half, lo=lo, rows=rows):
                        ctx[rows, lo + j * width // 2:lo + (j + 1) * width // 2] = half
                    read = lambda at, u=u: (lambda: kv[slot, u, :, at:at + width])
                    units.append((lambda lo=lo, rows=rows: qkv[rows, lo:lo + width], read(lo), read(d + lo), allowed, store))
            attend_all(units, head_dim, AHEAD_C)

        loader.need(8 * l + 6)
        every = slice(None)
        add_dot(hid, ctx, co.at[l], hid, every)
        loader.need(8 * l + 7)
        up(norm(hid[...]), w1.at[l], inner, every)
        loader.need(8 * l + 8)
        add_dot(hid, inner, w2.at[l], hid, every)
    out[...] = hid[...]


def decode(lens, nblk, y, kv, weights, seq, dec_len, head_dim, chunk, first_row, rows):
    d = y.shape[1]
    ff = weights[6].shape[2]
    skip = first_row * dec_len // chunk
    return pl.pallas_call(
        functools.partial(dec_kernel, head_dim, seq, dec_len, first_row),
        grid_spec=pltpu.PrefetchScalarGridSpec(
            num_scalar_prefetch=2, grid=(rows * dec_len // chunk,),
            in_specs=[pl.BlockSpec((chunk, d), lambda t, *_: (t + skip, 0))] + [ANY] * 9,
            out_specs=pl.BlockSpec((chunk, d), lambda t, *_: (t, 0)),
            scratch_shapes=[pltpu.VMEM(w.shape, BF) for w in weights]
            + [pltpu.VMEM((chunk, d), BF), pltpu.VMEM((chunk, 3 * d), BF), pltpu.VMEM((chunk, d), BF), pltpu.VMEM((chunk, ff), BF),
               pltpu.VMEM((2, PAIR, seq, 2 * d), BF),
               pltpu.SemaphoreType.DMA((8 * weights[0].shape[0],)), pltpu.SemaphoreType.DMA((2, PAIR))]),
        out_shape=jax.ShapeDtypeStruct((rows * dec_len, d), BF),
        cost_estimate=pl.CostEstimate(flops=rows * dec_len * 12_000_000 * 4, bytes_accessed=100_000_000, transcendentals=0),
        compiler_params=params(), name="decoder",
    )(lens, nblk, y, kv, *weights)


def solution(mesh):
    pair_size = mesh.shape["pair"]
    to_partner = [(source, (source + pair_size // 2) % pair_size) for source in range(pair_size)]
    row_spec = P(("data", "pair"))

    def per_device(x_enc, enc_len, y_dec, enc_wq, enc_wk, enc_wv, enc_wo, enc_w1, enc_w2, dec_wq, dec_wk, dec_wv, dec_wo, crs_wq, crs_wk, crs_wv, crs_wo, dec_w1, dec_w2):
        rows, seq, d = x_enc.shape
        dec_len = y_dec.shape[1]
        head_dim = enc_wo.shape[2]
        flat = lambda w: w.reshape(w.shape[0], w.shape[1] * w.shape[2], w.shape[3])
        enc_wo, dec_wo, crs_wo = flat(enc_wo), flat(dec_wo), flat(crs_wo)
        y_in = lax.ppermute(y_dec.reshape(rows * dec_len, d), "pair", to_partner)

        nblk = (enc_len + BLK - 1) // BLK
        ends = jnp.cumsum(nblk)
        starts = ends - nblk
        total = ends[-1]
        blk = jnp.arange(rows * seq // BLK, dtype=jnp.int32)
        row_of = jnp.minimum(jnp.sum((ends[None, :] <= blk[:, None]).astype(jnp.int32), axis=1), rows - 1)
        first = jnp.sum(jnp.where(row_of[:, None] == jnp.arange(rows)[None, :], starts[None, :], 0), axis=1)
        src = jnp.where(blk < total, row_of * (seq // BLK) + blk - first, 0)
        meta = jnp.stack([(total * BLK + TOK - 1) // TOK, total])


        x_flat = x_enc.reshape(rows * seq, d)
        n_enc = enc_wq.shape[0]
        qkv, h = pack(src, meta, x_flat, (enc_wq, enc_wk, enc_wv))
        for l in range(n_enc):
            ctx = attend_rows(starts, nblk, enc_len, qkv, seq, head_dim)
            if l + 1 < n_enc:
                h, qkv = mid(l, l + 1, meta, ctx, h, enc_wo, enc_w1, enc_w2, enc_wq, enc_wk, enc_wv)
            else:
                kv = last(l, src, meta, ctx, h, enc_wo, enc_w1, enc_w2, crs_wk, crs_wv, rows * seq)
        done, parts = 0, []
        for count in (rows - rows // 4, rows // 4):
            z = decode(enc_len, nblk, y_in, kv, (dec_wq, dec_wk, dec_wv, dec_wo, crs_wq, crs_wo, dec_w1, dec_w2), seq, dec_len, head_dim, CHUNK * dec_len, done, count)
            parts.append(lax.ppermute(z, "pair", to_partner))
            done += count
        return jnp.concatenate(parts, axis=0).reshape(y_dec.shape)

    return jax.shard_map(per_device, mesh=mesh, in_specs=(row_spec,) * 3 + (P(),) * 16, out_specs=row_spec, check_vma=False)
```

```python
import functools
import math

import jax
import jax.numpy as jnp
from jax import lax
from jax.experimental import pallas as pl
from jax.experimental.pallas import tpu as pltpu
from jax.sharding import PartitionSpec as P

BF = jnp.bfloat16
F32 = jnp.float32
BLK = 16
TOK = 512
QC = 128
CH = 256
AHEAD = 1
AHEAD_S = 2
AHEAD_C = 7
PAIR = 4
GRP = 128
CHUNK = 8
VMEM_LIMIT = 67_043_328
ANY = pl.BlockSpec(memory_space=pl.ANY)


def params(**kw):
    return pltpu.CompilerParams(vmem_limit_bytes=VMEM_LIMIT, **kw)


def dot(a, b):
    return jnp.dot(a, b, preferred_element_type=F32)


def norm(hidden):
    wide = hidden.astype(F32)
    inv = lax.rsqrt(jnp.mean(wide * wide, axis=-1, keepdims=True) + 1e-6)
    return (wide * inv).astype(BF)


def gelu(v):
    return jax.nn.gelu(v, approximate=True)


def quad_masks(head_dim):
    width = 4 * head_dim
    lane = lax.broadcasted_iota(jnp.int32, (1, width), 1) // head_dim
    return [(lane == h).astype(F32).astype(BF) for h in range(4)]


def quad_scores(q, k, head_dim):
    stacked = jnp.concatenate([q * mask for mask in quad_masks(head_dim)], axis=0)
    return lax.dot_general(stacked, k, (((1,), (1,)), ((), ())), preferred_element_type=F32)


def quad_context(s, v, allowed, head_dim):
    m = s.shape[0] // 4
    s = jnp.where(allowed, s, -1e30)
    top = jnp.max(s, axis=-1, keepdims=True)
    p = jnp.exp2((s - top) * (head_dim ** -0.5 * math.log2(math.e)))
    inv = 1.0 / jnp.sum(p, axis=-1, keepdims=True)
    o = dot(p.astype(BF), v)
    low = lax.broadcasted_iota(jnp.int32, (m, 2 * head_dim), 1) < head_dim
    halves = []
    for j in range(2):
        cols = slice(2 * head_dim * j, 2 * head_dim * (j + 1))
        first = o[2 * j * m:(2 * j + 1) * m, cols] * inv[2 * j * m:(2 * j + 1) * m]
        second = o[(2 * j + 1) * m:(2 * j + 2) * m, cols] * inv[(2 * j + 1) * m:(2 * j + 2) * m]
        halves.append(jnp.where(low, first, second).astype(BF))
    return halves


def attend_all(units, head_dim, ahead):
    held = {}
    for i in range(len(units) + ahead):
        if i < len(units):
            q, k = units[i][:2]
            held[i] = quad_scores(q(), k(), head_dim)
        if i >= ahead:
            v, allowed, store = units[i - ahead][2:]
            for j, half in enumerate(quad_context(held.pop(i - ahead), v(), allowed, head_dim)):
                store(j, half)


class Loader:
    def __init__(self, srcs, dsts, sems, ahead):
        self.loads = [pltpu.make_async_copy(s, d, sems.at[i]) for i, (s, d) in enumerate(zip(srcs, dsts))]
        self.ahead, self.started, self.waited = ahead, 0, 0
        self.first = pl.program_id(0) == 0

    def start(self, upto):
        for i in range(self.started, min(upto, len(self.loads))):
            self.loads[i].start()
        self.started = max(self.started, min(upto, len(self.loads)))

    def need(self, upto):
        @pl.when(self.first)
        def _():
            self.start(upto)
            for i in range(self.waited, upto):
                self.loads[i].wait()
            self.start(upto + self.ahead)
        self.waited = upto


def pack_kernel(layer, src, meta, x_hbm, wq, wk, wv, qkv_out, xp_out, xbuf, sem):
    t, n = pl.program_id(0), meta[0]
    per = TOK // BLK

    def fetch(tile, slot):
        @pl.loop(0, per)
        def _(i):
            row = pl.multiple_of(src[tile * per + i] * BLK, BLK)
            dst = pl.multiple_of(i * BLK, BLK)
            pltpu.make_async_copy(x_hbm.at[pl.ds(row, BLK)], xbuf.at[slot, pl.ds(dst, BLK)], sem.at[slot]).start()

    @pl.when(t == 0)
    def _():
        fetch(0, 0)

    @pl.when(t + 1 < n)
    def _():
        fetch(t + 1, (t + 1) % 2)

    @pl.when(t < n)
    def _():
        slot = t % 2
        pltpu.make_async_copy(x_hbm.at[pl.ds(0, TOK)], xbuf.at[slot], sem.at[slot]).wait()
        xp_out[...] = xbuf[slot]

        def run(part, _):
            project(norm(xbuf[slot, part, :]), (wq, wk, wv), qkv_out, part)

        by_fill(t, meta[1], run)


def by_fill(t, total, run):
    whole = (t + 1) * TOK - TOK // 2 < total * BLK

    @pl.when(whole)
    def _():
        run(slice(0, TOK), True)

    @pl.when(jnp.logical_not(whole))
    def _():
        run(slice(0, TOK // 2), False)


def project(normed, weights, out, part=slice(None)):
    width = weights[0].shape[1]
    for i, w in enumerate(weights):
        for c in range(0, width, CH):
            out[part, i * width + c:i * width + c + CH] = dot(normed, w[:, c:c + CH]).astype(BF)


def layer_spec(layer, d0, d1):
    return pl.BlockSpec((None, d0, d1), lambda *_: (layer, 0, 0), pipeline_mode=pl.Buffered(1))


def pack(src, meta, x, weights):
    cap, d = x.shape
    width = weights[0].shape[2]
    tile = lambda t, s, m: (jnp.minimum(t, m[0] - 1), 0)
    return pl.pallas_call(
        functools.partial(pack_kernel, 0),
        grid_spec=pltpu.PrefetchScalarGridSpec(
            num_scalar_prefetch=2, grid=(cap // TOK,),
            in_specs=[ANY] + [layer_spec(0, d, width)] * 3,
            out_specs=[pl.BlockSpec((TOK, 3 * width), tile), pl.BlockSpec((TOK, d), tile)],
            scratch_shapes=[pltpu.VMEM((2, TOK, d), BF), pltpu.SemaphoreType.DMA((2,))]),
        out_shape=[jax.ShapeDtypeStruct((cap + TOK, 3 * width), BF), jax.ShapeDtypeStruct((cap + TOK, d), BF)],
        compiler_params=params(), name="pack_project",
    )(src, meta, x, *weights)


def pieces(count, make):
    for size in (16, 8, 4, 2, 1):
        @pl.when((count & size) != 0)
        def _(size=size):
            make(count - (count & (2 * size - 1)), size)


def rows_kernel(head_dim, seq, starts, nblk, lens, qkv_hbm, ctx_hbm, buf, out, sem, osem):
    r, n = pl.program_id(0), pl.num_programs(0)
    d = out.shape[-1]

    def fetch(row, slot):
        return pltpu.make_async_copy(qkv_hbm.at[pl.ds(pl.multiple_of(starts[row] * BLK, BLK), seq)], buf.at[slot], sem.at[slot])

    def put(row, slot, first, size):
        to = pl.multiple_of((starts[row] + first) * BLK, BLK)
        frm = pl.multiple_of(first * BLK, BLK)
        return pltpu.make_async_copy(out.at[slot, pl.ds(frm, size * BLK)], ctx_hbm.at[pl.ds(to, size * BLK)], osem.at[slot])

    def drain(row, slot):
        pieces(nblk[row], lambda first, size: put(row, slot, first, size).wait())

    @pl.when(r == 0)
    def _():
        fetch(0, 0).start()

    @pl.when(r + 1 < n)
    def _():
        fetch(r + 1, (r + 1) % 2).start()

    slot = r % 2

    @pl.when(r >= 2)
    def _():
        drain(r - 2, slot)

    fetch(r, slot).wait()
    length = lens[r]

    @pl.when(starts[r] + seq // BLK > starts[n - 1] + nblk[n - 1])
    def _():
        keep = lax.broadcasted_iota(jnp.int32, (seq, d), 0) < length
        buf[slot, :, 2 * d:3 * d] = jnp.where(keep, buf[slot, :, 2 * d:3 * d], jnp.zeros((), BF))

    width = 4 * head_dim

    @pl.loop(0, (length + QC - 1) // QC)
    def _(c):
        rows = pl.ds(pl.multiple_of(c * QC, QC), QC)
        allowed = lax.broadcasted_iota(jnp.int32, (1, seq), 1) < length
        units = []
        for g in range(d // width):
            def store(j, half, lo=g * width):
                out[slot, rows, lo + j * width // 2:lo + (j + 1) * width // 2] = half
            lo = g * width
            units.append((lambda lo=lo: buf[slot, rows, lo:lo + width], lambda lo=lo: buf[slot, :, d + lo:d + lo + width],
                          lambda lo=lo: buf[slot, :, 2 * d + lo:2 * d + lo + width], allowed, store))
        attend_all(units, head_dim, AHEAD)

    pieces(nblk[r], lambda first, size: put(r, slot, first, size).start())

    @pl.when(r == n - 1)
    def _():
        drain(r - 1, 1 - slot)
        drain(r, slot)


def attend_rows(starts, nblk, lens, qkv, seq, head_dim):
    d = qkv.shape[1] // 3
    return pl.pallas_call(
        functools.partial(rows_kernel, head_dim, seq),
        grid_spec=pltpu.PrefetchScalarGridSpec(
            num_scalar_prefetch=3, grid=(lens.shape[0],), in_specs=[ANY], out_specs=ANY,
            scratch_shapes=[pltpu.VMEM((2, seq, 3 * d), BF), pltpu.VMEM((2, seq, d), BF),
                            pltpu.SemaphoreType.DMA((2,)), pltpu.SemaphoreType.DMA((2,))]),
        out_shape=jax.ShapeDtypeStruct((qkv.shape[0], d), BF),
        compiler_params=params(), name="row_attention",
    )(starts, nblk, lens, qkv)


def up(normed, w1, inner, part):
    for c in range(0, w1.shape[1], CH):
        inner[part, c:c + CH] = gelu(dot(normed, w1[:, c:c + CH])).astype(BF)


def add_dot(base, source, w, hid, part):
    for c in range(0, hid.shape[1], CH):
        hid[part, c:c + CH] = (base[part, c:c + CH].astype(F32) + dot(source[part, :], w[:, c:c + CH])).astype(BF)


def dense_part(part, ctx, x, wo, w1, w2, hid, inner, nxt, out, need):
    need(0)
    add_dot(x, ctx, wo, hid, part)
    need(1)
    up(norm(hid[part, :]), w1, inner, part)
    need(2)
    add_dot(hid, inner, w2, hid, part)
    need(3)
    project(norm(hid[part, :]), nxt, out, part)


def mid_kernel(layer, nxt, meta, ctx, x, wo_h, w1_h, w2_h, wq_h, wk_h, wv_h, h_out, qkv_out, wo, w1, w2, wq, wk, wv, inner, sem):
    t, n = pl.program_id(0), meta[0]
    loader = Loader([wo_h.at[layer], w1_h.at[layer], w2_h.at[layer], wq_h.at[nxt], wk_h.at[nxt], wv_h.at[nxt]], [wo, w1, w2, wq, wk, wv], sem, 4)

    @pl.when(t == 0)
    def _():
        loader.start(2)

    counts = [1, 2, 3, 6]

    def run(part, whole):
        dense_part(part, ctx, x, wo, w1, w2, h_out, inner, (wq, wk, wv), qkv_out, lambda i: loader.need(counts[i]) if whole else None)

    @pl.when(t < n)
    def _():
        by_fill(t, meta[1], run)


def mid(layer, nxt, meta, ctx, x, wo, w1, w2, wq, wk, wv):
    cap, d = x.shape
    ff, width = w1.shape[2], wq.shape[2]
    tile = lambda t, m: (jnp.minimum(t, m[0] - 1), 0)
    return pl.pallas_call(
        functools.partial(mid_kernel, layer, nxt),
        grid_spec=pltpu.PrefetchScalarGridSpec(
            num_scalar_prefetch=1, grid=(cap // TOK - 1,),
            in_specs=[pl.BlockSpec((TOK, d), tile), pl.BlockSpec((TOK, d), tile)] + [ANY] * 6,
            out_specs=[pl.BlockSpec((TOK, d), tile), pl.BlockSpec((TOK, 3 * width), tile)],
            scratch_shapes=[pltpu.VMEM((d, d), BF), pltpu.VMEM((d, ff), BF), pltpu.VMEM((ff, d), BF)] + [pltpu.VMEM((d, width), BF)] * 3
            + [pltpu.VMEM((TOK, ff), BF), pltpu.SemaphoreType.DMA((6,))]),
        out_shape=[jax.ShapeDtypeStruct((cap, d), BF), jax.ShapeDtypeStruct((cap, 3 * width), BF)],
        compiler_params=params(), name="mid_dense",
    )(meta, ctx, x, wo, w1, w2, wq, wk, wv)


def last_kernel(layer, n_dec, src, meta, ctx, x, wo_h, w1_h, w2_h, ck_h, cv_h, kv_hbm, wo, w1, w2, ckv, hid, inner, kv, sem, osem):
    t, n, total = pl.program_id(0), meta[0], meta[1]
    per = TOK // BLK
    crs = [h.at[l] for l in range(n_dec) for h in (ck_h, cv_h)]
    nxt = [ckv.at[i] for i in range(2 * n_dec)]
    loader = Loader([wo_h.at[layer], w1_h.at[layer], w2_h.at[layer]] + crs, [wo, w1, w2] + nxt, sem, 4)

    @pl.when(t == 0)
    def _():
        loader.start(2)

    def put(tile, i):
        to = pl.multiple_of(src[tile * per + i] * BLK, BLK)
        return pltpu.make_async_copy(kv.at[pl.ds(pl.multiple_of(i * BLK, BLK), BLK)], kv_hbm.at[pl.ds(to, BLK)], osem)

    def drain(tile):
        @pl.loop(0, jnp.minimum(per, total - tile * per))
        def _(i):
            put(tile, i).wait()

    counts = [1, 2, 3, 3 + 2 * n_dec]

    def run(part, whole):
        def need(i):
            if whole:
                loader.need(counts[i])
            if i == 3:
                @pl.when(t > 0)
                def _():
                    drain(t - 1)

        dense_part(part, ctx, x, wo, w1, w2, hid, inner, nxt, kv, need)

    @pl.when(t < n)
    def _():
        by_fill(t, total, run)

        @pl.loop(0, jnp.minimum(per, total - t * per))
        def _(i):
            put(t, i).start()

        @pl.when(t == n - 1)
        def _():
            drain(t)


def last(layer, src, meta, ctx, x, wo, w1, w2, ck, cv, slots):
    cap, d = x.shape
    n_dec, ff, width = ck.shape[0], w1.shape[2], ck.shape[2]
    tile = lambda t, s, m: (jnp.minimum(t, m[0] - 1), 0)
    return pl.pallas_call(
        functools.partial(last_kernel, layer, n_dec),
        grid_spec=pltpu.PrefetchScalarGridSpec(
            num_scalar_prefetch=2, grid=(slots // TOK,),
            in_specs=[pl.BlockSpec((TOK, d), tile), pl.BlockSpec((TOK, d), tile)] + [ANY] * 5,
            out_specs=ANY,
            scratch_shapes=[pltpu.VMEM((d, d), BF), pltpu.VMEM((d, ff), BF), pltpu.VMEM((ff, d), BF), pltpu.VMEM((2 * n_dec, d, width), BF),
                            pltpu.VMEM((TOK, d), BF), pltpu.VMEM((TOK, ff), BF), pltpu.VMEM((TOK, 2 * n_dec * width), BF),
                            pltpu.SemaphoreType.DMA((3 + 2 * n_dec,)), pltpu.SemaphoreType.DMA]),
        out_shape=jax.ShapeDtypeStruct((slots, 2 * n_dec * width), BF),
        compiler_params=params(), name="last_dense",
    )(src, meta, ctx, x, wo, w1, w2, ck, cv)


def dec_kernel(head_dim, seq, dec_len, first_row, lens, nblk, y, kv_hbm, *refs):
    hbm_w, refs = refs[:8], refs[8:]
    out, refs = refs[0], refs[1:]
    vmem_w, (hid, qkv, ctx, inner, kv, sem, ksem) = refs[:8], refs[8:]
    n_dec = vmem_w[0].shape[0]
    t = pl.program_id(0)
    m, d = hid.shape
    per = m // dec_len
    width = 4 * head_dim
    srcs, dsts = [], []
    for l in range(n_dec):
        srcs += [h.at[l] for h in hbm_w]
        dsts += [v.at[l] for v in vmem_w]
    loader = Loader(srcs, dsts, sem, 3)

    def fetch(l, pair, slot, act):
        for u in range(PAIR):
            row = first_row + t * per + pair * PAIR + u

            def one(first, size, row=row, u=u):
                frm = pl.multiple_of(row * seq + first * BLK, BLK)
                to = pl.multiple_of(first * BLK, BLK)
                getattr(pltpu.make_async_copy(kv_hbm.at[pl.ds(frm, size * BLK), pl.ds(2 * d * l, 2 * d)], kv.at[slot, u, pl.ds(to, size * BLK)], ksem.at[slot, u]), act)()

            pieces(nblk[row], one)

    @pl.when(t == 0)
    def _():
        loader.start(5)
        kv[...] = jnp.zeros_like(kv)

    hid[...] = y[...]
    row_q = lax.broadcasted_iota(jnp.int32, (4 * GRP, GRP), 0) % GRP
    col_k = lax.broadcasted_iota(jnp.int32, (4 * GRP, GRP), 1)
    causal = (row_q >= col_k) & (row_q // dec_len == col_k // dec_len)
    wq, wk, wv, wo, cq, co, w1, w2 = vmem_w
    for l in range(n_dec):
        fetch(l, 0, 0, "start")
        loader.need(8 * l + 3)
        project(norm(hid[...]), (wq.at[l], wk.at[l], wv.at[l]), qkv)
        units = []
        for lo in range(0, d, width):
            for r0 in range(0, m, GRP):
                def store(j, half, lo=lo, r0=r0):
                    ctx[r0:r0 + GRP, lo + j * width // 2:lo + (j + 1) * width // 2] = half
                read = lambda at, r0=r0: (lambda: qkv[r0:r0 + GRP, at:at + width])
                units.append((read(lo), read(d + lo), read(2 * d + lo), causal, store))
        attend_all(units, head_dim, AHEAD_S)
        loader.need(8 * l + 5)
        for c in range(0, d, CH):
            hid[:, c:c + CH] = (hid[:, c:c + CH].astype(F32) + dot(ctx[...], wo[l, :, c:c + CH])).astype(BF)
        project(norm(hid[...]), (cq.at[l],), qkv)

        @pl.loop(0, per // PAIR)
        def _(i):
            slot = i % 2

            @pl.when(i + 1 < per // PAIR)
            def _():
                fetch(l, i + 1, 1 - slot, "start")

            fetch(l, i, slot, "wait")
            units = []
            for u in range(PAIR):
                length = lens[first_row + t * per + i * PAIR + u]
                allowed = lax.broadcasted_iota(jnp.int32, (1, seq), 1) < length
                rows = pl.ds(pl.multiple_of((i * PAIR + u) * dec_len, dec_len), dec_len)
                for lo in range(0, d, width):
                    def store(j, half, lo=lo, rows=rows):
                        ctx[rows, lo + j * width // 2:lo + (j + 1) * width // 2] = half
                    read = lambda at, u=u: (lambda: kv[slot, u, :, at:at + width])
                    units.append((lambda lo=lo, rows=rows: qkv[rows, lo:lo + width], read(lo), read(d + lo), allowed, store))
            attend_all(units, head_dim, AHEAD_C)

        loader.need(8 * l + 6)
        every = slice(None)
        add_dot(hid, ctx, co.at[l], hid, every)
        loader.need(8 * l + 7)
        up(norm(hid[...]), w1.at[l], inner, every)
        loader.need(8 * l + 8)
        add_dot(hid, inner, w2.at[l], hid, every)
    out[...] = hid[...]


def decode(lens, nblk, y, kv, weights, seq, dec_len, head_dim, chunk, first_row, rows):
    d = y.shape[1]
    ff = weights[6].shape[2]
    skip = first_row * dec_len // chunk
    return pl.pallas_call(
        functools.partial(dec_kernel, head_dim, seq, dec_len, first_row),
        grid_spec=pltpu.PrefetchScalarGridSpec(
            num_scalar_prefetch=2, grid=(rows * dec_len // chunk,),
            in_specs=[pl.BlockSpec((chunk, d), lambda t, *_: (t + skip, 0))] + [ANY] * 9,
            out_specs=pl.BlockSpec((chunk, d), lambda t, *_: (t, 0)),
            scratch_shapes=[pltpu.VMEM(w.shape, BF) for w in weights]
            + [pltpu.VMEM((chunk, d), BF), pltpu.VMEM((chunk, 3 * d), BF), pltpu.VMEM((chunk, d), BF), pltpu.VMEM((chunk, ff), BF),
               pltpu.VMEM((2, PAIR, seq, 2 * d), BF),
               pltpu.SemaphoreType.DMA((8 * weights[0].shape[0],)), pltpu.SemaphoreType.DMA((2, PAIR))]),
        out_shape=jax.ShapeDtypeStruct((rows * dec_len, d), BF),
        cost_estimate=pl.CostEstimate(flops=rows * dec_len * 12_000_000 * 4, bytes_accessed=100_000_000, transcendentals=0),
        compiler_params=params(), name="decoder",
    )(lens, nblk, y, kv, *weights)


def solution(mesh):
    pair_size = mesh.shape["pair"]
    to_partner = [(source, (source + pair_size // 2) % pair_size) for source in range(pair_size)]
    row_spec = P(("data", "pair"))

    def per_device(x_enc, enc_len, y_dec, enc_wq, enc_wk, enc_wv, enc_wo, enc_w1, enc_w2, dec_wq, dec_wk, dec_wv, dec_wo, crs_wq, crs_wk, crs_wv, crs_wo, dec_w1, dec_w2):
        rows, seq, d = x_enc.shape
        dec_len = y_dec.shape[1]
        head_dim = enc_wo.shape[2]
        flat = lambda w: w.reshape(w.shape[0], w.shape[1] * w.shape[2], w.shape[3])
        enc_wo, dec_wo, crs_wo = flat(enc_wo), flat(dec_wo), flat(crs_wo)
        y_in = lax.ppermute(y_dec.reshape(rows * dec_len, d), "pair", to_partner)

        nblk = (enc_len + BLK - 1) // BLK
        ends = jnp.cumsum(nblk)
        starts = ends - nblk
        total = ends[-1]
        blk = jnp.arange(rows * seq // BLK, dtype=jnp.int32)
        row_of = jnp.minimum(jnp.sum((ends[None, :] <= blk[:, None]).astype(jnp.int32), axis=1), rows - 1)
        first = jnp.sum(jnp.where(row_of[:, None] == jnp.arange(rows)[None, :], starts[None, :], 0), axis=1)
        src = jnp.where(blk < total, row_of * (seq // BLK) + blk - first, 0)
        meta = jnp.stack([(total * BLK + TOK - 1) // TOK, total])


        x_flat = x_enc.reshape(rows * seq, d)
        n_enc = enc_wq.shape[0]
        qkv, h = pack(src, meta, x_flat, (enc_wq, enc_wk, enc_wv))
        for l in range(n_enc):
            ctx = attend_rows(starts, nblk, enc_len, qkv, seq, head_dim)
            if l + 1 < n_enc:
                h, qkv = mid(l, l + 1, meta, ctx, h, enc_wo, enc_w1, enc_w2, enc_wq, enc_wk, enc_wv)
            else:
                kv = last(l, src, meta, ctx, h, enc_wo, enc_w1, enc_w2, crs_wk, crs_wv, rows * seq)
        done, parts = 0, []
        for count in (rows - rows // 4, rows // 4):
            z = decode(enc_len, nblk, y_in, kv, (dec_wq, dec_wk, dec_wv, dec_wo, crs_wq, crs_wo, dec_w1, dec_w2), seq, dec_len, head_dim, CHUNK * dec_len, done, count)
            parts.append(lax.ppermute(z, "pair", to_partner))
            done += count
        return jnp.concatenate(parts, axis=0).reshape(y_dec.shape)

    return jax.shard_map(per_device, mesh=mesh, in_specs=(row_spec,) * 3 + (P(),) * 16, out_specs=row_spec, check_vma=False)
```
